32 devices in a mesh: gx: 2 (over y), gz: 4 (over x, core), ga: 4 (over z).
Axes of the slice: x: 2, y: 2, z: 4, core: 2. Of those that a mesh axis runs over, the one named last changes fastest.
Arguments:
- right_side: float32 [32, 128, 512], P('gx', 'ga', 'gz'), may hold values from -60 to 60, as said below
- diagonal: float32 [32, 128, 512], P('gx', 'ga', 'gz'), may hold values from 0.02 to 1
- element_features: bfloat16 [256, 4096], P(None, ('gx', 'gz', 'ga')), may hold values from -6 to 6
- sample_bank: bfloat16 [256, 131072], P(None, ('gx', 'gz', 'ga')), may hold values from -6 to 6
- target_bank: bfloat16 [6, 131072], P(None, ('gx', 'gz', 'ga')), may hold values from -6 to 6
- patch_index: int32 [65536], P(('gx', 'gz', 'ga')), may hold values from 0 to 4095
- w_first: bfloat16 [256, 256], replicated, may hold values from -0.375 to 0.375
- w_second: bfloat16 [256, 256], replicated, may hold values from -0.375 to 0.375
- w_third: bfloat16 [6, 256], replicated, may hold values from -0.375 to 0.375
Outputs:
- pressure: float32 [32, 128, 512], P('gx', 'ga', 'gz')
- residual: float32 [32, 128, 512], P('gx', 'ga', 'gz')
- step_first: float32 [256, 256], replicated
- step_second: float32 [256, 256], replicated
- step_third: float32 [6, 256], replicated
The draws below stay inside these ranges and needn't reach their ends.
Inputs may be any that keep to these rules, and one draw needn't show every extreme that they name: `right_side`: grows in magnitude along the first dimension. `patch_index`: each entry names a column of the sample_bank and target_bank block that lies on the same device as the entry.
All inputs are finite; a program needn't handle non-finite values.
Results may differ from the reference program's by a relative error of at most 0.0004.
The reference program's roundings to bfloat16 on the way count: a program that leaves them out, or rounds other values in their place, can miss the bound.
Values sent between devices are 32-bit elements; how exact they have to be, the bound alone decides.
A program may use at most 64 MiB of HBM per device.

```python
import math
import jax
import jax.numpy as jnp
from jax import lax

CX = 16
CY = 32
CZ = 128
EL = 8
CH = 256
STRESS = 6
ITERS = 12
SAMPLES_DEV = 2048
BANK_DEV = 4096
NX = 32
NY = 128
NZ = 512
ELEMS = 4096
BANK = 131072
SAMPLES = 65536
N_GX = 2
N_GZ = 4
N_GA = 4


def draw_right_side(key, part):
    position = jnp.arange(NX, dtype=jnp.float32) / NX
    growth = jnp.power(10.0, position)[:, None, None]
    random_part = jax.random.truncated_normal(key, -6.0, 6.0, (NX, NY, NZ), jnp.float32)
    return random_part * growth


def with_ends(result, key, low, high):
    longest = result.shape.index(max(result.shape))
    spots = []
    for shift in (0, 1):
        where = [jax.random.randint(jax.random.fold_in(key, axis), (), 0, length) for axis, length in enumerate(result.shape)]
        where[longest] = (where[longest] + shift) % result.shape[longest]
        spots.append(tuple(where))
    return result.at[spots[0]].set(low).at[spots[1]].set(high)


def level_of(own_key, dims, split, smallest, top_value):
    def one(axis_at, blocks):
        heights = jax.random.uniform(jax.random.fold_in(jax.random.fold_in(own_key, 6), axis_at), (blocks,), jnp.float32, smallest / len(split), top_value / len(split))
        return jnp.repeat(jnp.exp(heights), dims[axis_at] // blocks).reshape((-1,) + (1,) * (len(dims) - axis_at - 1))

    factor_of = one(*split[0])
    for cut in split[1:]:
        factor_of = factor_of * one(*cut)
    return factor_of


def scatter_about(rng, dims, scale, reach, cuts=(), kind=jnp.bfloat16):
    gain = level_of(rng, dims, cuts, -0.22, 0.18) if cuts else 1.0
    entries = jax.random.normal(rng, dims, jnp.float32) * scale * gain
    return jnp.minimum(jnp.maximum(entries, -reach), reach).astype(kind)


def setup_inputs(seed: int = 0) -> dict:
    arg_keys = jax.random.split(jax.random.key(seed), 10)
    return {
        "right_side": draw_right_side(jax.random.fold_in(arg_keys[9], 71), 0),
        "diagonal": jnp.clip(jnp.exp(math.log(1.0) - 3.912023 * jax.random.uniform(arg_keys[1], (NX, NY, NZ), jnp.float32) ** level_of(arg_keys[1], (NX, NY, NZ), ((0, 2), (1, 4), (2, 4)), -0.2, 0.2)), 0.02, 1.0),
        "element_features": scatter_about(arg_keys[2], (CH, ELEMS), 1.0, 6.0, ((1, 32),)),
        "sample_bank": scatter_about(arg_keys[3], (CH, BANK), 1.0, 6.0, ((1, 32),)),
        "target_bank": scatter_about(arg_keys[4], (STRESS, BANK), 1.0, 6.0, ((1, 32),)),
        "patch_index": with_ends(jax.random.randint(arg_keys[5], (SAMPLES,), 0, BANK_DEV), jax.random.fold_in(arg_keys[5], 1), 0, BANK_DEV - 1).astype(jnp.int32),
        "w_first": scatter_about(arg_keys[6], (CH, CH), CH ** -0.5, 0.375),
        "w_second": scatter_about(arg_keys[7], (CH, CH), CH ** -0.5, 0.375),
        "w_third": scatter_about(arg_keys[8], (STRESS, CH), CH ** -0.5, 0.375),
    }


taps = (1.6, -0.2, 8.0 / 315.0, -1.0 / 560.0)
center = 3.0 * 205.0 / 72.0
epsilon = 1e-06

def neighbours(padded):
    length_x = padded.shape[0] - 8
    length_y = padded.shape[1] - 8
    length_z = padded.shape[2] - 8
    summed = jnp.zeros((length_x, length_y, length_z), padded.dtype)
    for offset in range(1, 5):
        weight = taps[offset - 1]
        along_x = padded[4 + offset:4 + offset + length_x, 4:4 + length_y, 4:4 + length_z] + padded[4 - offset:4 - offset + length_x, 4:4 + length_y, 4:4 + length_z]
        along_y = padded[4:4 + length_x, 4 + offset:4 + offset + length_y, 4:4 + length_z] + padded[4:4 + length_x, 4 - offset:4 - offset + length_y, 4:4 + length_z]
        along_z = padded[4:4 + length_x, 4:4 + length_y, 4 + offset:4 + offset + length_z] + padded[4:4 + length_x, 4:4 + length_y, 4 - offset:4 - offset + length_z]
        summed = summed + weight * (along_x + along_y + along_z)
    return summed

def operate(padded, precond):
    return precond * padded[4:-4, 4:-4, 4:-4] - neighbours(padded)

def closure(w_first, w_second, w_third, inputs):
    linear_first = jnp.dot(w_first, inputs, preferred_element_type=jnp.float32)
    hidden_first = jax.nn.silu(linear_first).astype(jnp.bfloat16)
    linear_second = jnp.dot(w_second, hidden_first, preferred_element_type=jnp.float32)
    hidden_second = jax.nn.silu(linear_second).astype(jnp.bfloat16)
    predicted = jnp.dot(w_third, hidden_second, preferred_element_type=jnp.float32)
    return (linear_first, hidden_first, linear_second, hidden_second, predicted)

def slope(linear):
    sigmoid = jax.nn.sigmoid(linear)
    return sigmoid * (1.0 + linear * (1.0 - sigmoid))

def gradients(w_first, w_second, w_third, inputs, targets):
    linear_first, hidden_first, linear_second, hidden_second, predicted = closure(w_first, w_second, w_third, inputs)
    error = (predicted - targets.astype(jnp.float32)).astype(jnp.bfloat16)
    contract = (((1,), (1,)), ((), ()))
    leading = (((0,), (0,)), ((), ()))
    grad_third = lax.dot_general(error, hidden_second, contract, preferred_element_type=jnp.float32)
    back_second = lax.dot_general(w_third, error, leading, preferred_element_type=jnp.float32)
    delta_second = (back_second * slope(linear_second)).astype(jnp.bfloat16)
    grad_second = lax.dot_general(delta_second, hidden_first, contract, preferred_element_type=jnp.float32)
    back_first = lax.dot_general(w_second, delta_second, leading, preferred_element_type=jnp.float32)
    delta_first = (back_first * slope(linear_first)).astype(jnp.bfloat16)
    grad_first = lax.dot_general(delta_first, inputs, contract, preferred_element_type=jnp.float32)
    return (grad_first, grad_second, grad_third)

def normalize(gradient):
    return gradient * lax.rsqrt(jnp.mean(gradient * gradient) + epsilon)

def reference(right_side, diagonal, element_features, sample_bank, target_bank, patch_index, w_first, w_second, w_third):
    predicted = closure(w_first, w_second, w_third, element_features)[4]
    trace = (predicted[0] + predicted[1] + predicted[2]) / 3.0
    elems_x = CX // EL
    elems_y = CY // EL
    elems_z = CZ // EL
    blocks = trace.reshape(N_GX, N_GZ, N_GA, elems_x, elems_y, elems_z)
    blocks = blocks.transpose(0, 3, 2, 4, 1, 5).reshape(N_GX * elems_x, N_GA * elems_y, N_GZ * elems_z)
    forcing = jnp.repeat(jnp.repeat(jnp.repeat(blocks, EL, 0), EL, 1), EL, 2)
    source = right_side + forcing
    precond = diagonal + center
    pressure = jnp.zeros_like(source)
    residual = source
    scaled = residual / precond
    direction = scaled
    product_now = jnp.sum(residual * scaled)
    for iteration in range(ITERS):
        image_dir = operate(jnp.pad(direction, 4), precond)
        step_len = product_now / jnp.sum(direction * image_dir)
        pressure = pressure + step_len * direction
        residual = residual - step_len * image_dir
        scaled = residual / precond
        product_next = jnp.sum(residual * scaled)
        direction = scaled + product_next / product_now * direction
        product_now = product_next

    def accumulate(device, running):
        sample_start = (device * SAMPLES_DEV).astype(jnp.int32)
        bank_start = (device * BANK_DEV).astype(jnp.int32)
        columns = lax.dynamic_slice_in_dim(patch_index, sample_start, SAMPLES_DEV)
        bank_shard = lax.dynamic_slice_in_dim(sample_bank, bank_start, BANK_DEV, 1)
        goal_shard = lax.dynamic_slice_in_dim(target_bank, bank_start, BANK_DEV, 1)
        inputs = jnp.take(bank_shard, columns, axis=1)
        targets = jnp.take(goal_shard, columns, axis=1)
        partial_value = gradients(w_first, w_second, w_third, inputs, targets)
        return tuple((before + after for before, after in zip(running, partial_value)))
    initial = (jnp.zeros((CH, CH), jnp.float32), jnp.zeros((CH, CH), jnp.float32), jnp.zeros((STRESS, CH), jnp.float32))
    grad_first, grad_second, grad_third = lax.fori_loop(0, N_GX * N_GZ * N_GA, accumulate, initial)
    return (pressure, residual, normalize(grad_first), normalize(grad_second), normalize(grad_third))
```

```python
import functools

import jax
import jax.numpy as jnp
from jax import lax
from jax.experimental import pallas as pl
from jax.experimental.pallas import tpu as pltpu
from jax.sharding import PartitionSpec as P

EL = 8
ITERS = 12
TILE = 512
PHASES = (("gx", "gz"), ("ga",))
AXES = ("gx", "gz", "ga")

taps = (1.6, -0.2, 8.0 / 315.0, -1.0 / 560.0)
center = 3.0 * 205.0 / 72.0
epsilon = 1e-06
MESH = pl.DeviceIdType.MESH
F32 = jnp.float32
BF16 = jnp.bfloat16


def dot(a, b, dims=((1,), (0,)), precision=None):
    return lax.dot_general(a, b, (dims, ((), ())), preferred_element_type=F32, precision=precision)


def sigmoid(v):
    return 1.0 / (1.0 + jnp.exp(-v))


def grad_kernel(bank, target, index, w1, w2, w3, g1, g2, g3, counts):
    step = pl.program_id(0)
    rows = TILE // 128

    @pl.when(step == 0)
    def _():
        samples = index.shape[1]
        groups = counts.shape[0]
        ids = index[...]
        high = lax.broadcasted_iota(jnp.int32, (groups, samples), 0) == (ids // 128)
        low = lax.broadcasted_iota(jnp.int32, (128, samples), 0) == (ids % 128)
        counts[...] = dot(
            jnp.where(high, 1.0, 0.0).astype(BF16),
            jnp.where(low, 1.0, 0.0).astype(BF16),
            ((1,), (1,)),
        )
        g1[...] = jnp.zeros_like(g1)
        g2[...] = jnp.zeros_like(g2)
        g3[...] = jnp.zeros_like(g3)

    weight = jnp.concatenate([counts[pl.ds(step * rows + j, 1), :] for j in range(rows)], axis=1)
    x = bank[...]
    a1, a2, a3 = w1[...], w2[...], w3[...]
    l1 = dot(a1, x)
    s1 = sigmoid(l1)
    h1 = (l1 * s1).astype(BF16)
    l2 = dot(a2, h1)
    s2 = sigmoid(l2)
    h2 = (l2 * s2).astype(BF16)
    error = (dot(a3, h2) - target[...].astype(F32)).astype(BF16)

    def weighted(delta, right):
        scaled = delta.astype(F32) * weight
        upper = scaled.astype(BF16)
        lower = (scaled - upper.astype(F32)).astype(BF16)
        return dot(upper, right, ((1,), (1,))) + dot(lower, right, ((1,), (1,)))

    g3[...] += weighted(error, h2)
    d2 = (dot(a3, error, ((0,), (0,))) * (s2 * (1.0 + l2 * (1.0 - s2)))).astype(BF16)
    g2[...] += weighted(d2, h1)
    d1 = (dot(a2, d2, ((0,), (0,))) * (s1 * (1.0 + l1 * (1.0 - s1)))).astype(BF16)
    g1[...] += weighted(d1, x)


def closure_gradients(bank, target, index, w1, w2, w3):
    ch, columns = bank.shape
    stress = target.shape[0]
    whole = pl.BlockSpec(memory_space=pltpu.VMEM)
    fixed = lambda shape: pl.BlockSpec(shape, lambda i: (0, 0))
    return pl.pallas_call(
        grad_kernel,
        grid=(columns // TILE,),
        in_specs=[
            pl.BlockSpec((ch, TILE), lambda i: (0, i)),
            pl.BlockSpec((stress, TILE), lambda i: (0, i)),
            whole,
            whole,
            whole,
            whole,
        ],
        out_specs=[fixed((ch, ch)), fixed((ch, ch)), fixed((stress, ch))],
        out_shape=[
            jax.ShapeDtypeStruct((ch, ch), F32),
            jax.ShapeDtypeStruct((ch, ch), F32),
            jax.ShapeDtypeStruct((stress, ch), F32),
        ],
        scratch_shapes=[pltpu.VMEM((columns // 128, 128), F32)],
        compiler_params=pltpu.CompilerParams(dimension_semantics=("arbitrary",)),
        cost_estimate=pl.CostEstimate(
            flops=14 * ch * ch * columns, bytes_accessed=2 * ch * columns, transcendentals=4 * ch * columns
        ),
    )(bank, target, index.reshape(1, -1), w1, w2, w3)


def shift_offsets(sizes):
    combos = [()]
    for n in sizes:
        combos = [c + (k,) for c in combos for k in range(n)]
    return combos[1:]


def solve_kernel(
    sizes, right, diag, feats, w1, w2, w3, press, resid,
    mp, nb, wv, zv, sv, pv, inv, yp, yr, zp, zr, ar_src, ar_dst,
    h_send, h_recv, a_send, a_recv,
):
    lx, ly, lz = right.shape
    pos = {a: lax.axis_index(a) for a in AXES}

    def coords(axes, offs, sign):
        out = {}
        for a, k in zip(axes, offs):
            n = sizes[a]
            c = pos[a] + (k if sign > 0 else n - k) if k else pos[a]
            out[a] = lax.rem(c, n) if k else c
        return out

    def flat(axes, at):
        value = 0
        for a in axes:
            value = value * sizes[a] + at[a]
        return value

    groups = []
    for axes in PHASES:
        me = flat(axes, pos)
        peers = []
        for offs in shift_offsets([sizes[a] for a in axes]):
            to = {**pos, **coords(axes, offs, 1)}
            source = flat(axes, coords(axes, offs, -1))
            peers.append((to, source))
        groups.append((me, peers))

    mp[...] = jnp.zeros_like(mp)
    yr[...] = jnp.zeros_like(yr)
    zr[...] = jnp.zeros_like(zr)

    barrier = pltpu.get_barrier_semaphore()
    total = 0
    for _, peers in groups:
        for to, _ in peers:
            pl.semaphore_signal(barrier, inc=1, device_id=to, device_id_type=MESH)
            total += 1
    pl.semaphore_wait(barrier, total)

    lane = lax.broadcasted_iota(jnp.int32, (ly, lz), 1)
    sub8 = lax.broadcasted_iota(jnp.int32, (8, lz), 0)
    row_lane = lax.broadcasted_iota(jnp.int32, (1, lz), 1)

    def halo_copies(par):
        out = []

        def add(axis, step, number, src, dst):
            copy = pltpu.make_async_remote_copy(
                src_ref=src,
                dst_ref=dst,
                send_sem=h_send.at[number],
                recv_sem=h_recv.at[par, number],
                device_id={**pos, axis: jnp.clip(pos[axis] + step, 0, sizes[axis] - 1)},
                device_id_type=MESH,
            )
            can_send = pos[axis] < sizes[axis] - 1 if step > 0 else pos[axis] > 0
            will_get = pos[axis] > 0 if step > 0 else pos[axis] < sizes[axis] - 1
            out.append((copy, can_send, will_get))

        rows = pl.ds(8, ly)
        if sizes["gx"] > 1:
            add("gx", 1, 0, mp.at[par, pl.ds(lx, 4), rows], mp.at[par, pl.ds(0, 4), rows])
            add("gx", -1, 1, mp.at[par, pl.ds(4, 4), rows], mp.at[par, pl.ds(lx + 4, 4), rows])
        if sizes["ga"] > 1:
            add("ga", 1, 2, yp.at[par], yr.at[par, 0])
            add("ga", -1, 3, yp.at[par], yr.at[par, 1])
        if sizes["gz"] > 1:
            add("gz", 1, 4, zp.at[par], zr.at[par, 0])
            add("gz", -1, 5, zp.at[par], zr.at[par, 1])
        return out

    def halo_start(par):
        for copy, can_send, _ in halo_copies(par):
            pl.when(can_send)(copy.start)

    def halo_wait(par):
        for copy, _, will_get in halo_copies(par):
            pl.when(will_get)(copy.wait_recv)

    def halo_sent(par):
        for copy, can_send, _ in halo_copies(par):
            pl.when(can_send)(copy.wait_send)

    bases = []
    base = 0
    for axes in PHASES:
        bases.append(base)
        n = 1
        for a in axes:
            n *= sizes[a]
        base += n

    def sum_copies(par, phase):
        me, peers = groups[phase]
        out = []
        for k, (to, source) in enumerate(peers):
            slot = bases[phase]
            send = pltpu.make_async_remote_copy(
                src_ref=ar_src.at[par, phase],
                dst_ref=ar_dst.at[par, slot + me],
                send_sem=a_send.at[slot + k],
                recv_sem=a_recv.at[par, slot + me],
                device_id=to,
                device_id_type=MESH,
            )
            receive = pltpu.make_async_remote_copy(
                src_ref=ar_src.at[par, phase],
                dst_ref=ar_dst.at[par, slot + source],
                send_sem=a_send.at[slot + k],
                recv_sem=a_recv.at[par, slot + source],
                device_id=to,
                device_id_type=MESH,
            )
            out.append((send, receive))
        return out

    def sum_start(par, phase, row):
        ar_src[par, phase] = row
        ar_dst[par, bases[phase] + groups[phase][0]] = row
        for send, _ in sum_copies(par, phase):
            send.start()

    def sum_wait(par, phase):
        count = len(groups[phase][1]) + 1
        for _, receive in sum_copies(par, phase):
            receive.wait_recv()
        return jnp.sum(ar_dst[par, pl.ds(bases[phase], count)], axis=0)

    def sums_sent(par):
        for phase in range(len(PHASES)):
            for send, _ in sum_copies(par, phase):
                send.wait_send()

    def stencil_local(par):
        for x in range(lx):
            v = mp[par, 4 + x, pl.ds(8, ly)]
            acc = None
            for k in range(1, 5):
                t = mp[par, 4 + x, pl.ds(8 + k, ly)] + mp[par, 4 + x, pl.ds(8 - k, ly)]
                if x + k < lx:
                    t = t + mp[par, 4 + x + k, pl.ds(8, ly)]
                if x - k >= 0:
                    t = t + mp[par, 4 + x - k, pl.ds(8, ly)]
                t = t + jnp.where(lane >= k, pltpu.roll(v, k, 1), 0.0)
                t = t + jnp.where(lane < lz - k, pltpu.roll(v, lz - k, 1), 0.0)
                t = taps[k - 1] * t
                acc = t if acc is None else acc + t
            nb[x] = acc

    def z_correction(par):
        h = jnp.where(lane % 8 < 4, zr[par, 0], zr[par, 1])
        acc = jnp.zeros((ly, lz), F32)
        place = lane % 8
        for k in range(1, 5):
            ahead = jnp.where((place >= 4) & (place - 4 < k), pltpu.roll(h, k, 1), 0.0)
            behind = jnp.where((place < 4) & (place >= 4 - k), pltpu.roll(h, lz - k, 1), 0.0)
            acc = acc + taps[k - 1] * (ahead + behind)
        return acc

    def corrected(par, x, zc):
        acc = nb[x]
        for k in range(1, 5):
            if x - k < 0:
                acc = acc + taps[k - 1] * mp[par, 4 + x - k, pl.ds(8, ly)]
            if x + k >= lx:
                acc = acc + taps[k - 1] * mp[par, 4 + x + k, pl.ds(8, ly)]
        z = pltpu.roll(zc, (2 * lz - 8 * x - 4) % lz, 1)
        acc = acc + jnp.where((lane < 4) | (lane >= lz - 4), z, 0.0)
        h = jnp.where(sub8 < 4, yr[par, 1, x], yr[par, 0, x])
        low = jnp.zeros((8, lz), F32)
        high = jnp.zeros((8, lz), F32)
        for k in range(1, 5):
            low = low + taps[k - 1] * jnp.where(sub8 < k, pltpu.roll(h, k, 0), 0.0)
            high = high + taps[k - 1] * jnp.where(sub8 >= 8 - k, pltpu.roll(h, 8 - k, 0), 0.0)
        parts = [acc[:8] + low] + ([acc[8:-8]] if ly > 16 else []) + [acc[-8:] + high]
        return jnp.concatenate(parts, axis=0)

    def publish(par, x, m, packed):
        mp[par, 4 + x, pl.ds(8, ly)] = m
        yp[par, x] = jnp.where(sub8 < 4, m[:8], m[-8:])
        turned = pltpu.roll(m, (8 * x + 4) % lz, 1)
        return jnp.where((lane >= 8 * x) & (lane < 8 * x + 8), turned, packed)

    def fold(v):
        v = jnp.sum(v, axis=0, keepdims=True)
        return v + pltpu.roll(v, lz // 2, 1)

    def pair_row(gamma, delta):
        return jnp.where(row_lane < lz // 2, fold(gamma), fold(delta))

    def unpair(row):
        gamma = jnp.sum(jnp.where(row_lane < lz // 2, row, 0.0), axis=1, keepdims=True)
        delta = jnp.sum(jnp.where(row_lane < lz // 2, 0.0, row), axis=1, keepdims=True)
        return jnp.broadcast_to(gamma, (1, lz)), jnp.broadcast_to(delta, (1, lz))

    hidden = dot(w1[...], feats[...])
    hidden = (hidden * sigmoid(hidden)).astype(BF16)
    hidden = dot(w2[...], hidden)
    hidden = (hidden * sigmoid(hidden)).astype(BF16)
    predicted = dot(w3[...], hidden)
    trace = (predicted[0:1] + predicted[1:2] + predicted[2:3]) / 3.0
    ex, ey, ez = lx // EL, ly // EL, lz // EL
    spread = jnp.where(
        lax.broadcasted_iota(jnp.int32, (lz, lz), 0) == lax.broadcasted_iota(jnp.int32, (lz, lz), 1) // EL,
        1.0,
        0.0,
    )
    lines = jnp.concatenate(
        [trace if e == 0 else pltpu.roll(trace, (lz - e * ez) % lz, 1) for e in range(ex * ey)], axis=0
    )
    forcing = dot(lines, spread, precision=lax.Precision.HIGHEST)
    packed = jnp.zeros((ly, lz), F32)
    for x in range(lx):
        line = forcing[(x // EL) * ey : (x // EL) * ey + ey]
        block = jnp.concatenate([jnp.broadcast_to(line[j : j + 1], (EL, lz)) for j in range(ey)], axis=0)
        source = right[x] + block
        scale = 1.0 / (diag[x] + center)
        inv[x] = scale
        resid[x] = source
        packed = publish(1, x, source * scale, packed)
    zp[1] = packed
    press[...] = jnp.zeros_like(press)
    zv[...] = jnp.zeros_like(zv)
    sv[...] = jnp.zeros_like(sv)
    pv[...] = jnp.zeros_like(pv)
    halo_start(1)
    stencil_local(1)
    halo_wait(1)
    zc = z_correction(1)
    packed = jnp.zeros((ly, lz), F32)
    gamma = jnp.zeros((ly, lz), F32)
    delta = jnp.zeros((ly, lz), F32)
    for x in range(lx):
        r = resid[x]
        scale = inv[x]
        u = r * scale
        w = r - corrected(1, x, zc)
        wv[x] = w
        gamma = gamma + r * u
        delta = delta + w * u
        packed = publish(0, x, w * scale, packed)
    zp[0] = packed
    halo_sent(1)

    def coefficients(first, gamma, delta, gamma_old, alpha_old):
        beta = jnp.where(first, 0.0, gamma / gamma_old)
        return beta, gamma / (delta - beta * gamma / alpha_old)

    def iteration(i, carry):
        gamma_old, alpha_old, row = carry
        par = lax.rem(i, 2)
        later = 1 - par
        sum_start(par, 0, row)
        halo_start(par)
        stencil_local(par)
        for phase in range(1, len(PHASES)):
            sum_start(par, phase, sum_wait(par, phase - 1))
        halo_wait(par)
        zc = z_correction(par)
        for x in range(lx):
            nb[x] = corrected(par, x, zc)
        gamma, delta = unpair(sum_wait(par, len(PHASES) - 1))
        beta, alpha = coefficients(i == 0, gamma, delta, gamma_old, alpha_old)
        packed = jnp.zeros((ly, lz), F32)
        gamma_sum = jnp.zeros((ly, lz), F32)
        delta_sum = jnp.zeros((ly, lz), F32)
        for x in range(lx):
            r, w, scale = resid[x], wv[x], inv[x]
            z = (w - nb[x]) + beta * zv[x]
            s = w + beta * sv[x]
            p = r * scale + beta * pv[x]
            zv[x] = z
            sv[x] = s
            pv[x] = p
            press[x] = press[x] + alpha * p
            r = r - alpha * s
            w = w - alpha * z
            resid[x] = r
            wv[x] = w
            u = r * scale
            gamma_sum = gamma_sum + r * u
            delta_sum = delta_sum + w * u
            packed = publish(later, x, w * scale, packed)
        zp[later] = packed
        halo_sent(par)
        sums_sent(par)
        return gamma, alpha, pair_row(gamma_sum, delta_sum)

    ones = jnp.ones((1, lz), F32)
    gamma_old, alpha_old, row = lax.fori_loop(
        0, ITERS - 1, iteration, (ones, ones, pair_row(gamma, delta))
    )
    par = (ITERS - 1) % 2
    sum_start(par, 0, row)
    for phase in range(1, len(PHASES)):
        sum_start(par, phase, sum_wait(par, phase - 1))
    gamma, delta = unpair(sum_wait(par, len(PHASES) - 1))
    beta, alpha = coefficients(ITERS == 1, gamma, delta, gamma_old, alpha_old)
    for x in range(lx):
        r = resid[x]
        s = wv[x] + beta * sv[x]
        p = r * inv[x] + beta * pv[x]
        press[x] = press[x] + alpha * p
        resid[x] = r - alpha * s
    sums_sent(par)


def pressure_solve(right_side, diagonal, feats, w1, w2, w3):
    sizes = {a: lax.axis_size(a) for a in AXES}
    lx, ly, lz = right_side.shape
    slots = 0
    for axes in PHASES:
        n = 1
        for a in axes:
            n *= sizes[a]
        slots += n
    field = pltpu.VMEM((lx, ly, lz), F32)
    vmem = pl.BlockSpec(memory_space=pltpu.VMEM)
    return pl.pallas_call(
        functools.partial(solve_kernel, sizes),
        out_shape=[jax.ShapeDtypeStruct((lx, ly, lz), F32)] * 2,
        in_specs=[vmem] * 6,
        out_specs=[vmem] * 2,
        scratch_shapes=[
            pltpu.VMEM((2, lx + 8, ly + 16, lz), F32),
            field, field, field, field, field, field,
            pltpu.VMEM((2, lx, 8, lz), F32),
            pltpu.VMEM((2, 2, lx, 8, lz), F32),
            pltpu.VMEM((2, ly, lz), F32),
            pltpu.VMEM((2, 2, ly, lz), F32),
            pltpu.VMEM((2, len(PHASES), 1, lz), F32),
            pltpu.VMEM((2, slots, 1, lz), F32),
            pltpu.SemaphoreType.DMA((6,)),
            pltpu.SemaphoreType.DMA((2, 6)),
            pltpu.SemaphoreType.DMA((slots,)),
            pltpu.SemaphoreType.DMA((2, slots)),
        ],
        compiler_params=pltpu.CompilerParams(collective_id=0, has_side_effects=True),
        cost_estimate=pl.CostEstimate(
            flops=60_000_000, bytes_accessed=200_000_000, transcendentals=0
        ),
    )(right_side, diagonal, feats, w1, w2, w3)


def normalize(gradient):
    return gradient * lax.rsqrt(jnp.mean(gradient * gradient) + epsilon)


def body(
    right_side, diagonal, element_features, sample_bank, target_bank, patch_index, w_first, w_second, w_third
):
    grads = closure_gradients(sample_bank, target_bank, patch_index, w_first, w_second, w_third)
    grads = lax.psum(tuple(grads), AXES)
    pressure, residual = pressure_solve(
        right_side, diagonal, element_features, w_first, w_second, w_third
    )
    steps = tuple(normalize(g) for g in grads)
    return (pressure, residual) + steps


def solution(mesh):
    return jax.shard_map(
        body,
        mesh=mesh,
        in_specs=(
            P("gx", "ga", "gz"),
            P("gx", "ga", "gz"),
            P(None, ("gx", "gz", "ga")),
            P(None, ("gx", "gz", "ga")),
            P(None, ("gx", "gz", "ga")),
            P(("gx", "gz", "ga")),
            P(),
            P(),
            P(),
        ),
        out_specs=(P("gx", "ga", "gz"), P("gx", "ga", "gz"), P(), P(), P()),
        check_vma=False,
    )
```

```python
import functools

import jax
import jax.numpy as jnp
from jax import lax
from jax.experimental import pallas as pl
from jax.experimental.pallas import tpu as pltpu
from jax.sharding import PartitionSpec as P

EL = 8
ITERS = 12
TILE = 512
PHASES = (("gx", "gz"), ("ga",))
AXES = ("gx", "gz", "ga")

taps = (1.6, -0.2, 8.0 / 315.0, -1.0 / 560.0)
center = 3.0 * 205.0 / 72.0
epsilon = 1e-06
MESH = pl.DeviceIdType.MESH
F32 = jnp.float32
BF16 = jnp.bfloat16


def dot(a, b, dims=((1,), (0,)), precision=None):
    return lax.dot_general(a, b, (dims, ((), ())), preferred_element_type=F32, precision=precision)


def sigmoid(v):
    return 1.0 / (1.0 + jnp.exp(-v))


def grad_kernel(bank, target, index, w1, w2, w3, grads, counts):
    step = pl.program_id(0)
    rows = TILE // 128

    @pl.when(step == 0)
    def _():
        samples = index.shape[1]
        groups = counts.shape[0]
        ids = index[...]
        high = lax.broadcasted_iota(jnp.int32, (groups, samples), 0) == (ids // 128)
        low = lax.broadcasted_iota(jnp.int32, (128, samples), 0) == (ids % 128)
        counts[...] = dot(
            jnp.where(high, 1.0, 0.0).astype(BF16),
            jnp.where(low, 1.0, 0.0).astype(BF16),
            ((1,), (1,)),
        )
        grads[...] = jnp.zeros_like(grads)

    weight = jnp.concatenate([counts[pl.ds(step * rows + j, 1), :] for j in range(rows)], axis=1)
    x = bank[...]
    ch = x.shape[0]
    stress = target.shape[0]
    a1, a2, a3 = w1[...], w2[...], w3[...]
    l1 = dot(a1, x)
    s1 = sigmoid(l1)
    h1 = (l1 * s1).astype(BF16)
    l2 = dot(a2, h1)
    s2 = sigmoid(l2)
    h2 = (l2 * s2).astype(BF16)
    error = (dot(a3, h2) - target[...].astype(F32)).astype(BF16)

    def weighted(delta, right):
        scaled = delta.astype(F32) * weight
        upper = scaled.astype(BF16)
        lower = (scaled - upper.astype(F32)).astype(BF16)
        return dot(upper, right, ((1,), (1,))) + dot(lower, right, ((1,), (1,)))

    grads[2 * ch : 2 * ch + stress] += weighted(error, h2)
    d2 = (dot(a3, error, ((0,), (0,))) * (s2 * (1.0 + l2 * (1.0 - s2)))).astype(BF16)
    grads[ch : 2 * ch] += weighted(d2, h1)
    d1 = (dot(a2, d2, ((0,), (0,))) * (s1 * (1.0 + l1 * (1.0 - s1)))).astype(BF16)
    grads[:ch] += weighted(d1, x)


def closure_gradients(bank, target, index, w1, w2, w3, rows):
    ch, columns = bank.shape
    stress = target.shape[0]
    whole = pl.BlockSpec(memory_space=pltpu.VMEM)
    fixed = lambda shape: pl.BlockSpec(shape, lambda i: (0, 0))
    return pl.pallas_call(
        grad_kernel,
        grid=(columns // TILE,),
        in_specs=[
            pl.BlockSpec((ch, TILE), lambda i: (0, i)),
            pl.BlockSpec((stress, TILE), lambda i: (0, i)),
            whole,
            whole,
            whole,
            whole,
        ],
        out_specs=fixed((rows, ch)),
        out_shape=jax.ShapeDtypeStruct((rows, ch), F32),
        scratch_shapes=[pltpu.VMEM((columns // 128, 128), F32)],
        compiler_params=pltpu.CompilerParams(dimension_semantics=("arbitrary",)),
        cost_estimate=pl.CostEstimate(
            flops=14 * ch * ch * columns, bytes_accessed=2 * ch * columns, transcendentals=4 * ch * columns
        ),
    )(bank, target, index.reshape(1, -1), w1, w2, w3)


def shift_offsets(sizes):
    combos = [()]
    for n in sizes:
        combos = [c + (k,) for c in combos for k in range(n)]
    return combos[1:]


def solve_kernel(
    sizes, right, diag, feats, w1, w2, w3, grads, press, resid, step1, step2, step3,
    mp, nb, wv, zv, sv, pv, inv, yp, yr, zp, zr, ar_src, ar_dst,
    first, held, second, owned, third, full, g_send, g_recv,
    h_send, h_recv, a_send, a_recv,
):
    lx, ly, lz = right.shape
    pos = {a: lax.axis_index(a) for a in AXES}

    def coords(axes, offs, sign):
        out = {}
        for a, k in zip(axes, offs):
            n = sizes[a]
            c = pos[a] + (k if sign > 0 else n - k) if k else pos[a]
            out[a] = lax.rem(c, n) if k else c
        return out

    def flat(axes, at):
        value = 0
        for a in axes:
            value = value * sizes[a] + at[a]
        return value

    groups = []
    for axes in PHASES:
        me = flat(axes, pos)
        peers = []
        for offs in shift_offsets([sizes[a] for a in axes]):
            to = {**pos, **coords(axes, offs, 1)}
            source = flat(axes, coords(axes, offs, -1))
            peers.append((to, source))
        groups.append((me, peers))

    nx, nz, na = sizes["gx"], sizes["gz"], sizes["ga"]
    share = grads.shape[0] // nz
    piece = share // na

    def block_of(iz, ia=None):
        if ia is None:
            return pl.ds(pl.multiple_of(iz * share, 8), share)
        return pl.ds(pl.multiple_of((iz * na + ia) * piece, 8), piece)

    def along(axis, k, sign):
        return coords((axis,), (k,), sign)[axis]

    def gather_copy(number, axis, k, src, dst):
        return pltpu.make_async_remote_copy(
            src_ref=src,
            dst_ref=dst,
            send_sem=g_send.at[number],
            recv_sem=g_recv.at[number],
            device_id={**pos, axis: along(axis, k, 1)},
            device_id_type=MESH,
        )

    def scatter_gz(k):
        return gather_copy(k - 1, "gz", k, grads.at[block_of(along("gz", k, 1))], first.at[k - 1])

    def scatter_ga(k):
        rows = pl.ds(pl.multiple_of(along("ga", k, 1) * piece, 8), piece)
        return gather_copy(nz - 1 + k - 1, "ga", k, held.at[rows], second.at[k - 1])

    def add_gx(k, sign=1):
        slot = pos["gx"] if sign > 0 else along("gx", k, -1)
        return gather_copy(nz + na - 2 + k - 1, "gx", k, owned, third.at[slot])

    def gather_ga(k, sign=1):
        at = pos["ga"] if sign > 0 else along("ga", k, -1)
        rows = block_of(pos["gz"], at)
        return gather_copy(nz + na + nx - 3 + k - 1, "ga", k, full.at[rows], full.at[rows])

    def gather_gz(k, sign=1):
        at = pos["gz"] if sign > 0 else along("gz", k, -1)
        rows = block_of(at)
        return gather_copy(nz + 2 * na + nx - 4 + k - 1, "gz", k, full.at[rows], full.at[rows])

    def gradient_prepare(i):
        @pl.when(i == 3)
        def _():
            total = grads[block_of(pos["gz"]), :]
            for k in range(1, nz):
                scatter_gz(k).wait_recv()
                total = total + first[k - 1]
            held[...] = total

        @pl.when(i == 4)
        def _():
            total = held[pl.ds(pl.multiple_of(pos["ga"] * piece, 8), piece), :]
            for k in range(1, na):
                scatter_ga(k).wait_recv()
                total = total + second[k - 1]
            owned[...] = total
            third[pos["gx"]] = total

        @pl.when(i == 5)
        def _():
            for k in range(1, nx):
                add_gx(k, -1).wait_recv()
            full[block_of(pos["gz"], pos["ga"]), :] = jnp.sum(third[...], axis=0)

        @pl.when(i == 6)
        def _():
            for k in range(1, na):
                gather_ga(k, -1).wait_recv()

    def gradient_send(i):
        for turn in range(3):

            @pl.when(i == turn)
            def _():
                for k in range(1 + turn, nz, 3):
                    scatter_gz(k).start()

            @pl.when(i == 6 + turn)
            def _():
                for k in range(1 + turn, nz, 3):
                    gather_gz(k).start()

        @pl.when(i == 3)
        def _():
            for k in range(1, na):
                scatter_ga(k).start()

        @pl.when(i == 4)
        def _():
            for k in range(1, nx):
                add_gx(k).start()

        @pl.when(i == 5)
        def _():
            for k in range(1, na):
                gather_ga(k).start()

    def gradient_finish():
        for k in range(1, nz):
            gather_gz(k, -1).wait_recv()
            scatter_gz(k).wait_send()
            gather_gz(k).wait_send()
        for k in range(1, na):
            scatter_ga(k).wait_send()
            gather_ga(k).wait_send()
        for k in range(1, nx):
            add_gx(k).wait_send()
        ch = step1.shape[0]
        start = 0
        for out in (step1, step2, step3):
            count = out.shape[0]
            value = full[start : start + count]
            squares = jnp.sum(jnp.sum(value * value, axis=0, keepdims=True), axis=1, keepdims=True)
            out[...] = value * lax.rsqrt(squares / (count * ch) + epsilon)
            start += count

    mp[...] = jnp.zeros_like(mp)
    yr[...] = jnp.zeros_like(yr)
    zr[...] = jnp.zeros_like(zr)

    barrier = pltpu.get_barrier_semaphore()
    total = 0
    for _, peers in groups:
        for to, _ in peers:
            pl.semaphore_signal(barrier, inc=1, device_id=to, device_id_type=MESH)
            total += 1
    pl.semaphore_wait(barrier, total)

    lane = lax.broadcasted_iota(jnp.int32, (ly, lz), 1)
    sub8 = lax.broadcasted_iota(jnp.int32, (8, lz), 0)
    row_lane = lax.broadcasted_iota(jnp.int32, (1, lz), 1)

    def halo_copies(par):
        out = []

        def add(axis, step, number, src, dst):
            copy = pltpu.make_async_remote_copy(
                src_ref=src,
                dst_ref=dst,
                send_sem=h_send.at[number],
                recv_sem=h_recv.at[par, number],
                device_id={**pos, axis: jnp.clip(pos[axis] + step, 0, sizes[axis] - 1)},
                device_id_type=MESH,
            )
            can_send = pos[axis] < sizes[axis] - 1 if step > 0 else pos[axis] > 0
            will_get = pos[axis] > 0 if step > 0 else pos[axis] < sizes[axis] - 1
            out.append((copy, can_send, will_get))

        rows = pl.ds(8, ly)
        if sizes["gx"] > 1:
            add("gx", 1, 0, mp.at[par, pl.ds(lx, 4), rows], mp.at[par, pl.ds(0, 4), rows])
            add("gx", -1, 1, mp.at[par, pl.ds(4, 4), rows], mp.at[par, pl.ds(lx + 4, 4), rows])
        if sizes["ga"] > 1:
            add("ga", 1, 2, yp.at[par], yr.at[par, 0])
            add("ga", -1, 3, yp.at[par], yr.at[par, 1])
        if sizes["gz"] > 1:
            add("gz", 1, 4, zp.at[par], zr.at[par, 0])
            add("gz", -1, 5, zp.at[par], zr.at[par, 1])
        return out

    def halo_start(par):
        for copy, can_send, _ in halo_copies(par):
            pl.when(can_send)(copy.start)

    def halo_wait(par):
        for copy, _, will_get in halo_copies(par):
            pl.when(will_get)(copy.wait_recv)

    def halo_sent(par):
        for copy, can_send, _ in halo_copies(par):
            pl.when(can_send)(copy.wait_send)

    bases = []
    base = 0
    for axes in PHASES:
        bases.append(base)
        n = 1
        for a in axes:
            n *= sizes[a]
        base += n

    def sum_copies(par, phase):
        me, peers = groups[phase]
        out = []
        for k, (to, source) in enumerate(peers):
            slot = bases[phase]
            send = pltpu.make_async_remote_copy(
                src_ref=ar_src.at[par, phase],
                dst_ref=ar_dst.at[par, slot + me],
                send_sem=a_send.at[slot + k],
                recv_sem=a_recv.at[par, slot + me],
                device_id=to,
                device_id_type=MESH,
            )
            receive = pltpu.make_async_remote_copy(
                src_ref=ar_src.at[par, phase],
                dst_ref=ar_dst.at[par, slot + source],
                send_sem=a_send.at[slot + k],
                recv_sem=a_recv.at[par, slot + source],
                device_id=to,
                device_id_type=MESH,
            )
            out.append((send, receive))
        return out

    def sum_start(par, phase, row):
        ar_src[par, phase] = row
        ar_dst[par, bases[phase] + groups[phase][0]] = row
        for send, _ in sum_copies(par, phase):
            send.start()

    def sum_wait(par, phase):
        count = len(groups[phase][1]) + 1
        for _, receive in sum_copies(par, phase):
            receive.wait_recv()
        return jnp.sum(ar_dst[par, pl.ds(bases[phase], count)], axis=0)

    def sums_sent(par):
        for phase in range(len(PHASES)):
            for send, _ in sum_copies(par, phase):
                send.wait_send()

    def stencil_local(par):
        for x in range(lx):
            v = mp[par, 4 + x, pl.ds(8, ly)]
            acc = None
            for k in range(1, 5):
                t = mp[par, 4 + x, pl.ds(8 + k, ly)] + mp[par, 4 + x, pl.ds(8 - k, ly)]
                if x + k < lx:
                    t = t + mp[par, 4 + x + k, pl.ds(8, ly)]
                if x - k >= 0:
                    t = t + mp[par, 4 + x - k, pl.ds(8, ly)]
                t = t + jnp.where(lane >= k, pltpu.roll(v, k, 1), 0.0)
                t = t + jnp.where(lane < lz - k, pltpu.roll(v, lz - k, 1), 0.0)
                t = taps[k - 1] * t
                acc = t if acc is None else acc + t
            nb[x] = acc

    def z_correction(par):
        h = jnp.where(lane % 8 < 4, zr[par, 0], zr[par, 1])
        acc = jnp.zeros((ly, lz), F32)
        place = lane % 8
        for k in range(1, 5):
            ahead = jnp.where((place >= 4) & (place - 4 < k), pltpu.roll(h, k, 1), 0.0)
            behind = jnp.where((place < 4) & (place >= 4 - k), pltpu.roll(h, lz - k, 1), 0.0)
            acc = acc + taps[k - 1] * (ahead + behind)
        return acc

    def corrected(par, x, zc):
        acc = nb[x]
        for k in range(1, 5):
            if x - k < 0:
                acc = acc + taps[k - 1] * mp[par, 4 + x - k, pl.ds(8, ly)]
            if x + k >= lx:
                acc = acc + taps[k - 1] * mp[par, 4 + x + k, pl.ds(8, ly)]
        z = pltpu.roll(zc, (2 * lz - 8 * x - 4) % lz, 1)
        acc = acc + jnp.where((lane < 4) | (lane >= lz - 4), z, 0.0)
        h = jnp.where(sub8 < 4, yr[par, 1, x], yr[par, 0, x])
        low = jnp.zeros((8, lz), F32)
        high = jnp.zeros((8, lz), F32)
        for k in range(1, 5):
            low = low + taps[k - 1] * jnp.where(sub8 < k, pltpu.roll(h, k, 0), 0.0)
            high = high + taps[k - 1] * jnp.where(sub8 >= 8 - k, pltpu.roll(h, 8 - k, 0), 0.0)
        parts = [acc[:8] + low] + ([acc[8:-8]] if ly > 16 else []) + [acc[-8:] + high]
        return jnp.concatenate(parts, axis=0)

    def publish(par, x, m, packed):
        mp[par, 4 + x, pl.ds(8, ly)] = m
        yp[par, x] = jnp.where(sub8 < 4, m[:8], m[-8:])
        turned = pltpu.roll(m, (8 * x + 4) % lz, 1)
        return jnp.where((lane >= 8 * x) & (lane < 8 * x + 8), turned, packed)

    def fold(v):
        v = jnp.sum(v, axis=0, keepdims=True)
        return v + pltpu.roll(v, lz // 2, 1)

    def pair_row(gamma, delta):
        return jnp.where(row_lane < lz // 2, fold(gamma), fold(delta))

    def unpair(row):
        gamma = jnp.sum(jnp.where(row_lane < lz // 2, row, 0.0), axis=1, keepdims=True)
        delta = jnp.sum(jnp.where(row_lane < lz // 2, 0.0, row), axis=1, keepdims=True)
        return jnp.broadcast_to(gamma, (1, lz)), jnp.broadcast_to(delta, (1, lz))

    hidden = dot(w1[...], feats[...])
    hidden = (hidden * sigmoid(hidden)).astype(BF16)
    hidden = dot(w2[...], hidden)
    hidden = (hidden * sigmoid(hidden)).astype(BF16)
    predicted = dot(w3[...], hidden)
    trace = (predicted[0:1] + predicted[1:2] + predicted[2:3]) / 3.0
    ex, ey, ez = lx // EL, ly // EL, lz // EL
    spread = jnp.where(
        lax.broadcasted_iota(jnp.int32, (lz, lz), 0) == lax.broadcasted_iota(jnp.int32, (lz, lz), 1) // EL,
        1.0,
        0.0,
    )
    lines = jnp.concatenate(
        [trace if e == 0 else pltpu.roll(trace, (lz - e * ez) % lz, 1) for e in range(ex * ey)], axis=0
    )
    forcing = dot(lines, spread, precision=lax.Precision.HIGHEST)
    packed = jnp.zeros((ly, lz), F32)
    for x in range(lx):
        line = forcing[(x // EL) * ey : (x // EL) * ey + ey]
        block = jnp.concatenate([jnp.broadcast_to(line[j : j + 1], (EL, lz)) for j in range(ey)], axis=0)
        source = right[x] + block
        scale = 1.0 / (diag[x] + center)
        inv[x] = scale
        resid[x] = source
        packed = publish(1, x, source * scale, packed)
    zp[1] = packed
    press[...] = jnp.zeros_like(press)
    zv[...] = jnp.zeros_like(zv)
    sv[...] = jnp.zeros_like(sv)
    pv[...] = jnp.zeros_like(pv)
    halo_start(1)
    stencil_local(1)
    halo_wait(1)
    zc = z_correction(1)
    packed = jnp.zeros((ly, lz), F32)
    gamma = jnp.zeros((ly, lz), F32)
    delta = jnp.zeros((ly, lz), F32)
    for x in range(lx):
        r = resid[x]
        scale = inv[x]
        u = r * scale
        w = r - corrected(1, x, zc)
        wv[x] = w
        gamma = gamma + r * u
        delta = delta + w * u
        packed = publish(0, x, w * scale, packed)
    zp[0] = packed
    halo_sent(1)

    def coefficients(first, gamma, delta, gamma_old, alpha_old):
        beta = jnp.where(first, 0.0, gamma / gamma_old)
        return beta, gamma / (delta - beta * gamma / alpha_old)

    def iteration(i, carry):
        gamma_old, alpha_old, row = carry
        par = lax.rem(i, 2)
        later = 1 - par
        sum_start(par, 0, row)
        halo_start(par)
        stencil_local(par)
        gradient_prepare(i)
        for phase in range(1, len(PHASES)):
            sum_start(par, phase, sum_wait(par, phase - 1))
        gradient_send(i)
        halo_wait(par)
        zc = z_correction(par)
        for x in range(lx):
            nb[x] = corrected(par, x, zc)
        gamma, delta = unpair(sum_wait(par, len(PHASES) - 1))
        beta, alpha = coefficients(i == 0, gamma, delta, gamma_old, alpha_old)
        packed = jnp.zeros((ly, lz), F32)
        gamma_sum = jnp.zeros((ly, lz), F32)
        delta_sum = jnp.zeros((ly, lz), F32)
        for x in range(lx):
            r, w, scale = resid[x], wv[x], inv[x]
            z = (w - nb[x]) + beta * zv[x]
            s = w + beta * sv[x]
            p = r * scale + beta * pv[x]
            zv[x] = z
            sv[x] = s
            pv[x] = p
            press[x] = press[x] + alpha * p
            r = r - alpha * s
            w = w - alpha * z
            resid[x] = r
            wv[x] = w
            u = r * scale
            gamma_sum = gamma_sum + r * u
            delta_sum = delta_sum + w * u
            packed = publish(later, x, w * scale, packed)
        zp[later] = packed
        halo_sent(par)
        sums_sent(par)
        return gamma, alpha, pair_row(gamma_sum, delta_sum)

    ones = jnp.ones((1, lz), F32)
    gamma_old, alpha_old, row = lax.fori_loop(
        0, ITERS - 1, iteration, (ones, ones, pair_row(gamma, delta))
    )
    par = (ITERS - 1) % 2
    sum_start(par, 0, row)
    gradient_finish()
    for phase in range(1, len(PHASES)):
        sum_start(par, phase, sum_wait(par, phase - 1))
    gamma, delta = unpair(sum_wait(par, len(PHASES) - 1))
    beta, alpha = coefficients(ITERS == 1, gamma, delta, gamma_old, alpha_old)
    for x in range(lx):
        r = resid[x]
        s = wv[x] + beta * sv[x]
        p = r * inv[x] + beta * pv[x]
        press[x] = press[x] + alpha * p
        resid[x] = r - alpha * s
    sums_sent(par)


def pressure_solve(right_side, diagonal, feats, w1, w2, w3, grads):
    sizes = {a: lax.axis_size(a) for a in AXES}
    lx, ly, lz = right_side.shape
    slots = 0
    for axes in PHASES:
        n = 1
        for a in axes:
            n *= sizes[a]
        slots += n
    nx, nz, na = (sizes[a] for a in ("gx", "gz", "ga"))
    rows, ch = grads.shape
    share = rows // nz
    piece = share // na
    copies = max(2 * (nz - 1) + 2 * (na - 1) + nx - 1, 1)
    field = pltpu.VMEM((lx, ly, lz), F32)
    vmem = pl.BlockSpec(memory_space=pltpu.VMEM)
    return pl.pallas_call(
        functools.partial(solve_kernel, sizes),
        out_shape=[jax.ShapeDtypeStruct((lx, ly, lz), F32)] * 2
        + [jax.ShapeDtypeStruct(w.shape, F32) for w in (w1, w2, w3)],
        in_specs=[vmem] * 7,
        out_specs=[vmem] * 5,
        scratch_shapes=[
            pltpu.VMEM((2, lx + 8, ly + 16, lz), F32),
            field, field, field, field, field, field,
            pltpu.VMEM((2, lx, 8, lz), F32),
            pltpu.VMEM((2, 2, lx, 8, lz), F32),
            pltpu.VMEM((2, ly, lz), F32),
            pltpu.VMEM((2, 2, ly, lz), F32),
            pltpu.VMEM((2, len(PHASES), 1, lz), F32),
            pltpu.VMEM((2, slots, 1, lz), F32),
            pltpu.VMEM((max(nz - 1, 1), share, ch), F32),
            pltpu.VMEM((share, ch), F32),
            pltpu.VMEM((max(na - 1, 1), piece, ch), F32),
            pltpu.VMEM((piece, ch), F32),
            pltpu.VMEM((nx, piece, ch), F32),
            pltpu.VMEM((rows, ch), F32),
            pltpu.SemaphoreType.DMA((copies,)),
            pltpu.SemaphoreType.DMA((copies,)),
            pltpu.SemaphoreType.DMA((6,)),
            pltpu.SemaphoreType.DMA((2, 6)),
            pltpu.SemaphoreType.DMA((slots,)),
            pltpu.SemaphoreType.DMA((2, slots)),
        ],
        compiler_params=pltpu.CompilerParams(collective_id=0, has_side_effects=True),
        cost_estimate=pl.CostEstimate(
            flops=60_000_000, bytes_accessed=200_000_000, transcendentals=0
        ),
    )(right_side, diagonal, feats, w1, w2, w3, grads)


def body(
    right_side, diagonal, element_features, sample_bank, target_bank, patch_index, w_first, w_second, w_third
):
    unit = 8 * lax.axis_size("gz") * lax.axis_size("ga")
    rows = w_first.shape[0] + w_second.shape[0] + w_third.shape[0]
    rows = (rows + unit - 1) // unit * unit
    grads = closure_gradients(
        sample_bank, target_bank, patch_index, w_first, w_second, w_third, rows
    )
    return tuple(
        pressure_solve(
            right_side, diagonal, element_features, w_first, w_second, w_third, grads
        )
    )


def solution(mesh):
    return jax.shard_map(
        body,
        mesh=mesh,
        in_specs=(
            P("gx", "ga", "gz"),
            P("gx", "ga", "gz"),
            P(None, ("gx", "gz", "ga")),
            P(None, ("gx", "gz", "ga")),
            P(None, ("gx", "gz", "ga")),
            P(("gx", "gz", "ga")),
            P(),
            P(),
            P(),
        ),
        out_specs=(P("gx", "ga", "gz"), P("gx", "ga", "gz"), P(), P(), P()),
        check_vma=False,
    )
```
